32 devices in a mesh: gx: 8 (over z, y), gy: 4 (over x, core).
Axes of the slice: x: 2, y: 2, z: 4, core: 2. Of those that a mesh axis runs over, the one named last changes fastest.
Arguments:
- probes: bfloat16 [16, 32768], P(None, ('gx', 'gy')), may hold values from -73 to 73, as said below
- previous: bfloat16 [16, 32768], P(None, ('gx', 'gy')), may hold values from -6 to 6
- prev_coupling: float32 [16, 16], replicated, may hold values from -1.5 to 1.5
- leaves: bfloat16 [32, 1024, 1024], P(('gx', 'gy')), may hold values from -1 to 3, as said below
- bases: bfloat16 [5, 64, 32768], P(None, None, ('gx', 'gy')), may hold values from -6 to 6
- leaf_sizes: int32 [32], P(('gx', 'gy')), may hold values from 1 to 1024, 24576 in all
Outputs:
- rayleigh: float32 [16, 16], replicated
- factor: float32 [16, 16], replicated
- next_block: float32 [16, 32768], P(None, ('gx', 'gy'))
The draws below stay inside these ranges and needn't reach their ends.
Inputs may be any that keep to these rules, and one draw needn't show every extreme that they name: For every probe p and slot s, |probes[p, s]| stays within the range below. Each leaves[i] is symmetric. `leaf_sizes`: the real points of a leaf fill its first slots; the sizes sum to 24576.
All inputs are finite; a program needn't handle non-finite values. No bound on the sum of `leaf_sizes` on one device may be relied on, other than what follows from the above.
Results may differ from the reference program's by a relative error of at most 0.0022.
Values sent between devices are 32-bit elements; how exact they have to be, the bound alone decides.
A program may use at most 64 MiB of HBM per device.

```python
import math
import jax
import jax.numpy as jnp
import numpy as np
from jax import lax

LEAF = 1024
RANK = 64
PROBES = 16
LEAVES = 32
NPTS = 32768
LEVELS = 5
FILLED = 24576


def draw_probes(key, part):
    base_key = jax.random.fold_in(key, 17)
    first, second, third = jax.random.split(base_key, 3)
    values = jax.random.truncated_normal(first, -4.0, 4.0, (PROBES, NPTS), jnp.float32)
    rows = 10.0 ** (jax.random.uniform(second, (NPTS,), jnp.float32) - 0.5)
    columns = 10.0 ** (jax.random.uniform(third, (PROBES,), jnp.float32) - 0.5)
    rising = 0.6 * (1.0 + 2.0 * jnp.arange(NPTS, dtype=jnp.float32) / NPTS)
    return (values * (rows * rising)[None, :] * columns[:, None]).astype(jnp.bfloat16)


def draw_leaves(key, part):
    base_key = jax.random.fold_in(key, 29)

    def one_leaf(index):
        leaf_key = jax.random.fold_in(base_key, index)
        raw = jax.random.truncated_normal(leaf_key, -4.0, 4.0, (LEAF, LEAF), jnp.float32)
        symmetric = (raw + raw.T) * (0.5 / LEAF ** 0.5)
        return (symmetric + 2.0 * jnp.eye(LEAF, dtype=jnp.float32)).astype(jnp.bfloat16)
    return lax.map(one_leaf, jnp.arange(LEAVES, dtype=jnp.int32))


def block_levels(stream_key, dims, cuts, low, high):
    def one(dim, shards_of):
        draws = jax.random.uniform(jax.random.fold_in(jax.random.fold_in(stream_key, 6), dim), (shards_of,), jnp.float32, low / len(cuts), high / len(cuts))
        return jnp.repeat(jnp.exp(draws), dims[dim] // shards_of).reshape((-1,) + (1,) * (len(dims) - dim - 1))

    level = one(*cuts[0])
    for cut in cuts[1:]:
        level = level * one(*cut)
    return level


def split_up(count, total, most, skew):
    weights = [(1 << 20) // math.isqrt(standing ** skew) + 1 for standing in range(2, count + 1)]
    rest, given = total - most - (count - 1), [1] * (count - 1)
    while rest > 0:
        movable = [i for i in range(count - 1) if given[i] < most]
        mass, budget = sum([weights[i] for i in movable]), rest
        for i in movable:
            extra = min(most - given[i], max(1, budget * weights[i] // mass), rest)
            given[i] = given[i] + extra
            rest = rest - extra
    return np.array([most] + given)


def ragged_sizes(key, count, total, bound, lean):
    if count == 2:
        one = jax.random.randint(key, (), max(1, total - bound), min(bound, total - 1) + 1)
        return jnp.stack([one, total - one])
    lengths = jnp.asarray(split_up(count, total, bound, lean), jnp.int32)
    twos = (count - 1) // 2
    source_of, taker = lengths[1:1 + 2 * twos:2], lengths[2:2 + 2 * twos:2]
    margin = jnp.minimum(source_of - 1, bound - taker)
    passed = jax.random.randint(jax.random.fold_in(key, 1), (twos,), 0, 1 << 20) % (margin + 1)
    lengths = lengths.at[1:1 + 2 * twos:2].set(source_of - passed).at[2:2 + 2 * twos:2].set(taker + passed)
    return lengths[jax.random.permutation(jax.random.fold_in(key, 2), count)]


def centred(stream_key, dims, scale, most, shards=(), kind=jnp.bfloat16):
    drawn = jax.random.normal(stream_key, dims, jnp.float32) * scale
    if len(shards) > 0:
        drawn = block_levels(stream_key, dims, shards, -0.22, 0.18) * drawn
    return jnp.clip(drawn, min=-most, max=most).astype(kind)


def setup_inputs(seed: int = 0) -> dict:
    seeds = jax.random.split(jax.random.key(seed), 7)
    return {
        "probes": draw_probes(jax.random.fold_in(seeds[6], 71), 0),
        "previous": centred(seeds[1], (PROBES, NPTS), 1.0, 6.0, ((1, 32),)),
        "prev_coupling": centred(seeds[2], (PROBES, PROBES), PROBES ** -0.5, 1.5, (), jnp.float32),
        "leaves": draw_leaves(jax.random.fold_in(seeds[6], 71), 0),
        "bases": centred(seeds[4], (LEVELS, RANK, NPTS), 1.0, 6.0, ((2, 32),)),
        "leaf_sizes": ragged_sizes(seeds[5], LEAVES, FILLED, LEAF, 1).astype(jnp.int32),
    }


def reference(probes, previous, prev_coupling, leaves, bases, leaf_sizes):
    highest = lax.Precision.HIGHEST
    valid = (jnp.arange(LEAF, dtype=jnp.int32)[None, :] < leaf_sizes[:, None]).reshape(NPTS)
    block = jnp.where(valid[None, :], probes, jnp.zeros_like(probes)).astype(jnp.float32)
    older = jnp.where(valid[None, :], previous, jnp.zeros_like(previous)).astype(jnp.float32)
    shaped = block.reshape(PROBES, LEAVES // 8, 8, LEAF).transpose(1, 2, 0, 3)
    grouped = leaves.reshape(LEAVES // 8, 8, LEAF, LEAF)

    def apply_group(pair):
        mats, vecs = pair
        return jnp.einsum('lrc,lpc->lpr', mats.astype(jnp.float32), vecs, precision=highest)
    image = lax.map(apply_group, (grouped, shaped))
    image = image.transpose(2, 0, 1, 3).reshape(PROBES, NPTS)
    for level in range(LEVELS):
        width = LEAF * 2 ** level
        nodes = NPTS // width
        basis = bases[level].astype(jnp.float32).reshape(RANK, nodes, width)
        pieces = block.reshape(PROBES, nodes, width)
        coef = jnp.einsum('pnm,rnm->pnr', pieces, basis, precision=highest)
        partner = coef.reshape(PROBES, nodes // 2, 2, RANK)[:, :, ::-1, :].reshape(PROBES, nodes, RANK)
        partner = (partner * (1.0 / math.sqrt(RANK * width))).astype(jnp.bfloat16).astype(jnp.float32)
        image = image + jnp.einsum('pnr,rnm->pnm', partner, basis, precision=highest).reshape(PROBES, NPTS)
    image = jnp.where(valid[None, :], image, jnp.zeros_like(image))
    inverse = 1.0 / FILLED
    rayleigh = jnp.dot(block, image.T, precision=highest) * inverse
    residual = image - jnp.dot(rayleigh.T, block, precision=highest) - jnp.dot(prev_coupling, older, precision=highest)
    gram = jnp.dot(residual, residual.T, precision=highest) * inverse
    factor = jnp.linalg.cholesky(gram)
    next_block = jax.scipy.linalg.solve_triangular(factor, residual, lower=True)
    return (rayleigh, factor, next_block)
```

```python
import functools
import math

import jax
import jax.numpy as jnp
from jax import lax
from jax.experimental import pallas as pl
from jax.experimental.pallas import tpu as pltpu
from jax.sharding import PartitionSpec as P

MESH = pl.DeviceIdType.MESH
F32 = jnp.float32
BF16 = jnp.bfloat16
NT = (((1,), (1,)), ((), ()))


def stages_of(spread):
    cuts = [0, min(3, spread)]
    while cuts[-1] < spread:
        cuts.append(min(cuts[-1] + 2, spread))
    return list(zip(cuts[:-1], cuts[1:]))


def tree(values):
    while len(values) > 1:
        values = [a + b for a, b in zip(values[::2], values[1::2])]
    return values[0]


def split3(value):
    high = value.astype(BF16)
    rest = value - high.astype(F32)
    middle = rest.astype(BF16)
    low = (rest - middle.astype(F32)).astype(BF16)
    return high, middle, low


def small_dot(a, b, transposed=False):
    dims = NT if transposed else (((1,), (0,)), ((), ()))
    return lax.dot_general(
        a, b, dims, precision=lax.Precision.HIGHEST, preferred_element_type=F32
    )


def kernel(
    spread, width, inverse,
    probes_hbm, previous_hbm, coupling_hbm, leaves_hbm, bases_hbm, sizes_hbm,
    rayleigh_ref, factor_ref, next_ref,
    probes, previous, coupling, leaves, bases, sizes, wide, local_sems, *rest,
):
    stages = stages_of(spread)
    count = len(stages)
    levels = spread
    runs, lands = rest[:count], rest[count : 2 * count]
    own2, land2 = rest[2 * count : 3 * count], rest[3 * count : 4 * count]
    sems = rest[4 * count :]
    send1, recv1, send2, recv2 = (sems[i * count : (i + 1) * count] for i in range(4))
    p_count, rows = probes.shape
    rank = bases.shape[1]
    half = p_count // 2

    me = lax.axis_index("gx") * width + lax.axis_index("gy")

    def device(mask):
        target = me
        for bit in range(spread):
            if mask >> bit & 1:
                target = target + (1 - 2 * (me // 2**bit % 2)) * 2**bit
        return (target // width, target % width)

    loads = []
    for i, (src, dst) in enumerate(
        [(sizes_hbm, sizes), (probes_hbm, probes), (bases_hbm, bases),
         (leaves_hbm, leaves), (previous_hbm, previous), (coupling_hbm, coupling)]
    ):
        load = pltpu.make_async_copy(src, dst, local_sems.at[i])
        load.start()
        loads.append(load)

    barrier = pltpu.get_barrier_semaphore()
    greeted = 0
    for low, high in stages:
        for m in range(1, 2 ** (high - low)):
            pl.semaphore_signal(barrier, inc=1, device_id=device(m << low), device_id_type=MESH)
            greeted += 1

    loads[0].wait()
    loads[1].wait()
    valid = lax.broadcasted_iota(jnp.int32, (p_count, rows), 1) < sizes[0]
    block = jnp.where(valid, probes[...].astype(F32), 0.0).astype(BF16)
    loads[2].wait()
    for level in range(levels):
        part = lax.dot_general(block, bases[level], NT, preferred_element_type=F32)
        runs[0][level] = jnp.concatenate([part[:half], part[half:]], axis=1)
    pl.semaphore_wait(barrier, greeted)

    def send_stage1(s):
        low, high = stages[s]
        copies = []
        for m in reversed(range(1, 2 ** (high - low))):
            top = low + m.bit_length() - 1
            pieces = [(top, 1, 0)]
            if high < levels:
                pieces.append((high, levels - high, 1))
            for src, size, dst in pieces:
                copy = pltpu.make_async_remote_copy(
                    src_ref=runs[s].at[pl.ds(src, size)],
                    dst_ref=lands[s].at[m - 1, pl.ds(dst, size)],
                    send_sem=send1[s].at[m - 1, min(dst, 1)],
                    recv_sem=recv1[s].at[m - 1, min(dst, 1)],
                    device_id=device(m << low),
                    device_id_type=MESH,
                )
                copy.start()
                copies.append(copy)
        return copies

    def scaled_partners(s):
        low, high = stages[s]
        found = []
        for t in range(low, high):
            b = t - low
            total = tree([lands[s][m - 1, 0] for m in range(2**b, 2 ** (b + 1))])
            total = total * (1.0 / math.sqrt(rank * rows * 2**t))
            found.append(jnp.concatenate([total[:, :rank], total[:, rank:]], axis=0).astype(BF16))
        return found

    copies = send_stage1(0)
    loads[4].wait()
    older = jnp.where(valid, previous[...].astype(F32), 0.0).astype(BF16)
    wide[3 * p_count : 4 * p_count, :] = block
    wide[4 * p_count : 5 * p_count, :] = older
    pair = wide[3 * p_count : 5 * p_count, :]
    early_b = lax.dot_general(block, pair, NT, preferred_element_type=F32)
    early_o = lax.dot_general(older, older, NT, preferred_element_type=F32)
    loads[3].wait()
    image = jnp.dot(block, leaves[0], preferred_element_type=F32)
    for s in range(count):
        low, high = stages[s]
        for copy in copies:
            copy.wait()
        if s + 1 < count:
            for t in range(high, levels):
                runs[s + 1][t] = tree(
                    [runs[s][t]]
                    + [lands[s][m - 1, 1 + t - high] for m in range(1, 2 ** (high - low))]
                )
            copies = send_stage1(s + 1)
        for t, scaled in zip(range(low, high), scaled_partners(s)):
            image = image + jnp.dot(scaled, bases[t], preferred_element_type=F32)
    image = jnp.where(valid, image, 0.0)
    high, middle, lowest = split3(image)
    wide[0:p_count, :] = high
    wide[p_count : 2 * p_count, :] = middle
    wide[2 * p_count : 3 * p_count, :] = lowest
    products = lax.dot_general(
        wide[0 : 3 * p_count, :], wide[...], NT, preferred_element_type=F32
    )
    products = (
        products[:p_count] + products[p_count : 2 * p_count] + products[2 * p_count :]
    )
    own2[0][...] = jnp.concatenate([products, early_b, early_o], axis=1)
    for s in range(count):
        low, top = stages[s]
        copies = []
        for m in reversed(range(1, 2 ** (top - low))):
            copy = pltpu.make_async_remote_copy(
                src_ref=own2[s],
                dst_ref=land2[s].at[m - 1],
                send_sem=send2[s].at[m - 1],
                recv_sem=recv2[s].at[m - 1],
                device_id=device(m << low),
                device_id_type=MESH,
            )
            copy.start()
            copies.append(copy)
        for copy in copies:
            copy.wait()
        total = tree([own2[s][...]] + [land2[s][m - 1] for m in range(1, 2 ** (top - low))])
        if s + 1 < count:
            own2[s + 1][...] = total
    total = total * inverse
    q = p_count
    square = total[:, :q] + total[:, q : 2 * q] + total[:, 2 * q : 3 * q]
    crossed = total[:, 3 * q : 5 * q]
    turned = total[:, 3 * q : 4 * q]
    loads[5].wait()
    mix = coupling[...]
    bb_bo = total[:, 5 * q : 7 * q]
    bo = total[:, 6 * q : 7 * q]
    oo = total[:, 7 * q : 8 * q]
    both = jnp.concatenate([turned, mix], axis=1)
    lower_part = jnp.concatenate([small_dot(mix, bo, True), small_dot(mix, oo)], axis=1)
    u = small_dot(turned, bb_bo) + lower_part
    gram = square - small_dot(both, crossed, True) + small_dot(u - crossed, both, True)
    row_ids = lax.broadcasted_iota(jnp.int32, (q, q), 0)
    lane_ids = lax.broadcasted_iota(jnp.int32, (q, q), 1)
    eye = jnp.where(row_ids == lane_ids, 1.0, 0.0).astype(F32)
    rayleigh_ref[...] = small_dot(eye, turned, True)
    work = jnp.concatenate([gram, eye, eye, eye, -turned, -mix], axis=1)
    factor = jnp.zeros((q, q), F32)
    wide_rows = lax.broadcasted_iota(jnp.int32, work.shape, 0)
    done = jnp.zeros_like(work)
    for k in range(q):
        scale = lax.rsqrt(work[k : k + 1, k : k + 1])
        row = work[k : k + 1, :] * scale
        column = work[:, k : k + 1] * scale
        factor = jnp.where((lane_ids == k) & (row_ids >= k), column, factor)
        done = jnp.where(wide_rows == k, row, done)
        work = work - column * row
    factor_ref[...] = factor
    mixing = done[:, q:]
    pieces = jnp.concatenate(list(split3(mixing)), axis=0)
    result = jnp.dot(pieces, wide[...], preferred_element_type=F32)
    next_ref[...] = result[:q] + result[q : 2 * q] + result[2 * q :]


def body(probes, previous, prev_coupling, leaves, bases, leaf_sizes):
    p_count, rows = probes.shape
    devices = lax.axis_size(("gx", "gy"))
    spread = devices.bit_length() - 1
    filled = devices * rows * 3 // 4
    stages = stages_of(spread)
    rank = bases.shape[1]
    tile = (p_count // 2, 2 * rank)
    lanes = 8 * p_count
    peers = [2 ** (high - low) - 1 for low, high in stages]
    dma = pltpu.SemaphoreType.DMA
    scratch = [
        pltpu.VMEM(probes.shape, BF16),
        pltpu.VMEM(previous.shape, BF16),
        pltpu.VMEM(prev_coupling.shape, F32),
        pltpu.VMEM(leaves.shape, BF16),
        pltpu.VMEM(bases.shape, BF16),
        pltpu.SMEM(leaf_sizes.shape, jnp.int32),
        pltpu.VMEM((5 * p_count, rows), BF16),
        dma((6,)),
    ]
    scratch += [pltpu.VMEM((spread,) + tile, F32) for _ in stages]
    scratch += [
        pltpu.VMEM((n, 1 + spread - high) + tile, F32) for n, (_, high) in zip(peers, stages)
    ]
    scratch += [pltpu.VMEM((p_count, lanes), F32) for _ in stages]
    scratch += [pltpu.VMEM((n, p_count, lanes), F32) for n in peers]
    scratch += [dma((n, 2)) for n in peers] * 2 + [dma((n,)) for n in peers] * 2
    return pl.pallas_call(
        functools.partial(kernel, spread, lax.axis_size("gy"), 1.0 / filled),
        out_shape=[
            jax.ShapeDtypeStruct((p_count, p_count), F32),
            jax.ShapeDtypeStruct((p_count, p_count), F32),
            jax.ShapeDtypeStruct((p_count, rows), F32),
        ],
        in_specs=[pl.BlockSpec(memory_space=pl.ANY)] * 6,
        out_specs=[pl.BlockSpec(memory_space=pltpu.VMEM)] * 3,
        scratch_shapes=scratch,
        compiler_params=pltpu.CompilerParams(collective_id=0, has_side_effects=True),
    )(probes, previous, prev_coupling, leaves, bases, leaf_sizes)


def solution(mesh):
    in_specs = (
        P(None, ("gx", "gy")),
        P(None, ("gx", "gy")),
        P(),
        P(("gx", "gy"), None, None),
        P(None, None, ("gx", "gy")),
        P(("gx", "gy")),
    )
    out_specs = (P(), P(), P(None, ("gx", "gy")))
    return jax.shard_map(body, mesh=mesh, in_specs=in_specs, out_specs=out_specs, check_vma=False)
```
